32 devices in a mesh: cell: 8 (over y, x, core), gene: 4 (over z).
Axes of the slice: x: 2, y: 2, z: 4, core: 2. Of those that a mesh axis runs over, the one named last changes fastest.
Arguments:
- counts: int32 [3072, 8192], P('gene', 'cell'), may hold values from 0 to 11
- batch_id: int32 [8192], P('cell'), may hold values from 0 to 63
- live_cells: int32 [8], P('cell'), may hold values from 256 to 1024, as said below
- knot_bin: int32 [8192], P('cell'), may hold values from 0 to 14
- depth_frac: float32 [8192], P('cell'), may hold values from 0 to 1
- cell_covariates: float32 [16, 8192], P(None, 'cell'), may hold values from -3 to 3
- coefficients: float32 [3072, 32], P('gene'), may hold values from -1.2 to 1.2
- batch_effect: float32 [3072, 64], P('gene'), may hold values from -1.8 to 1.8
- factors: bfloat16 [8192, 64], P('cell'), may hold values from -4 to 4
- loadings: bfloat16 [3072, 64], P('gene'), may hold values from -0.19921875 to 0.19921875
Outputs:
- beta_step: float32 [3072, 32], P('gene')
- factor_step: float32 [8192, 64], P('cell')
- loading_score: float32 [3072, 64], P('gene')
The draws below stay inside these ranges and needn't reach their ends.
Inputs may be any that keep to these rules, and one draw needn't show every extreme that they name: `live_cells`: each index of the cell axis has its live cells in its first slots, at least 256 of them; some index is full in every draw.
All inputs are finite; a program needn't handle non-finite values.
Results may differ from the reference program's by a relative error of at most 0.0003.
Values sent between devices are 32-bit elements; how exact they have to be, the bound alone decides.
A program may use at most 64 MiB of HBM per device.

```python
import math
import jax
import jax.numpy as jnp
import numpy as np
from jax import lax

GENES = 3072
SPL = 16
COV = 16
FACTORS = 64
BATCHES = 64
CDEV = 1024
COVARS = 32
CELLS = 8192
NSHARD = 8
N_GENE = 4


def draw_live_cells(key, part):
    first_key, second_key = jax.random.split(jax.random.fold_in(key, 17))
    ladder = jax.random.randint(first_key, (NSHARD,), 0, 65)
    quarter = CDEV // 4
    live_count = quarter + (CDEV - quarter) * ladder * ladder // 4096
    chosen = jax.random.randint(second_key, (), 0, NSHARD)
    return jnp.where(jnp.arange(NSHARD, dtype=jnp.int32) == chosen, CDEV, live_count).astype(jnp.int32)


def set_ends(drawn, own_key, low, top_value):
    longest = drawn.shape.index(max(drawn.shape))
    spots = []
    for shift in (0, 1):
        where = [jax.random.randint(jax.random.fold_in(own_key, axis), (), 0, length) for axis, length in enumerate(drawn.shape)]
        where[longest] = (where[longest] + shift) % drawn.shape[longest]
        spots.append(tuple(where))
    return drawn.at[spots[0]].set(low).at[spots[1]].set(top_value)


def level_of(key, dims, cuts, low, largest):
    def one(position, shards_of):
        heights = jax.random.uniform(jax.random.fold_in(jax.random.fold_in(key, 6), position), (shards_of,), jnp.float32, low / len(cuts), largest / len(cuts))
        return jnp.repeat(jnp.exp(heights), dims[position] // shards_of).reshape((-1,) + (1,) * (len(dims) - position - 1))

    level = one(*cuts[0])
    for cut in cuts[1:]:
        level = level * one(*cut)
    return level


def rank_bounds(count, slope):
    loads = [(1 << 20) // math.isqrt(rank ** slope) + 1 for rank in range(1, count + 1)]
    scale = 1 + sum(loads) // (1 << 30)
    return np.cumsum(np.array([max(1, weight // scale) for weight in loads]))


def ranked_ids(stream_key, shape, amount, skew):
    listing = rank_bounds(amount, skew)
    lot = jax.random.randint(jax.random.fold_in(stream_key, 1), shape, 0, int(listing[amount - 1]))
    rank = jnp.searchsorted(jnp.asarray(listing, jnp.int32), lot, side="right")
    return jax.random.permutation(jax.random.fold_in(stream_key, 2), amount)[rank].astype(jnp.int32)


def scatter_about(rng, dims, deviation, most, cuts=(), kind=jnp.bfloat16):
    result = jax.random.normal(rng, dims, jnp.float32) * deviation
    if len(cuts) > 0:
        result = level_of(rng, dims, cuts, -0.22, 0.18) * result
    return jnp.clip(result, min=-most, max=most).astype(kind)


def setup_inputs(seed: int = 0) -> dict:
    splits = jax.random.split(jax.random.key(seed), 11)
    counts = set_ends(ranked_ids(splits[0], (GENES, CELLS), 12, 2), jax.random.fold_in(splits[0], 3), 0, 11).astype(jnp.int32)
    batch_id = set_ends(jax.random.randint(splits[1], (CELLS,), 0, BATCHES), jax.random.fold_in(splits[1], 1), 0, BATCHES - 1).astype(jnp.int32)
    live_cells = draw_live_cells(jax.random.fold_in(splits[10], 71), 0)
    knot_bin = set_ends(jax.random.randint(splits[3], (CELLS,), 0, SPL - 1), jax.random.fold_in(splits[3], 1), 0, (SPL - 1) - 1).astype(jnp.int32)
    depth_frac = jnp.clip(1.0 * jax.random.uniform(splits[4], (CELLS,), jnp.float32) ** level_of(splits[4], (CELLS,), ((0, 8),), -0.2, 0.2), 0.0, 1.0)
    cell_covariates = scatter_about(splits[5], (COV, CELLS), 0.5, 3.0, ((1, 8),), jnp.float32)
    coefficients = scatter_about(splits[6], (GENES, COVARS), 0.2, 1.2, ((0, 4),), jnp.float32)
    batch_effect = scatter_about(splits[7], (GENES, BATCHES), 0.3, 1.8, ((0, 4),), jnp.float32)
    factors = scatter_about(splits[8], (CELLS, FACTORS), 1.0, 4.0, ((0, 8),))
    loadings = scatter_about(splits[9], (GENES, FACTORS), 0.05, 0.19921875, ((0, 4),))
    return dict(counts=counts, batch_id=batch_id, live_cells=live_cells, knot_bin=knot_bin, depth_frac=depth_frac, cell_covariates=cell_covariates, coefficients=coefficients, batch_effect=batch_effect, factors=factors, loadings=loadings)


ridge_weight = 1.0

def design_rows(knot_bin, depth_frac, cell_covariates):
    levels = jnp.arange(SPL, dtype=jnp.int32)[:, None]
    fraction = depth_frac[None, :]
    hat_basis = jnp.where(levels == knot_bin[None, :], 1.0 - fraction, 0.0)
    hat_basis = hat_basis + jnp.where(levels == knot_bin[None, :] + 1, fraction, 0.0)
    return jnp.concatenate([hat_basis.astype(cell_covariates.dtype), cell_covariates], axis=0)

def newton_solve(gram_flat, score):
    columns = score.shape[-1]
    identity = jnp.eye(columns, dtype=gram_flat.dtype)
    system = gram_flat.reshape(-1, columns, columns) + ridge_weight * identity
    factor_lower = jnp.linalg.cholesky(system)
    middle = jax.scipy.linalg.solve_triangular(factor_lower, score[..., None], lower=True)
    return jax.scipy.linalg.solve_triangular(factor_lower, middle, lower=True, trans=1)[..., 0]

def reference(counts, batch_id, live_cells, knot_bin, depth_frac, cell_covariates, coefficients, batch_effect, factors, loadings):
    highest = lax.Precision.HIGHEST
    contract = (((1,), (1,)), ((), ()))
    totals = lax.optimization_barrier(jnp.sum(counts, axis=0)).astype(jnp.float32)
    offset = jnp.log((1.0 + totals) / GENES)
    positions = jnp.arange(CELLS, dtype=jnp.int32)
    live_mask = (positions % CDEV < live_cells[positions // CDEV]).astype(jnp.float32)
    design = design_rows(knot_bin, depth_frac, cell_covariates)
    columns = design.shape[0]
    pairs = (design[:, None, :] * design[None, :, :]).reshape(columns * columns, CELLS)
    onehot = (jnp.arange(BATCHES, dtype=jnp.int32)[:, None] == batch_id[None, :]).astype(jnp.float32)
    stacked = jnp.concatenate([design, onehot], axis=0)
    factors_wide = factors.astype(jnp.float32)
    gene_block = GENES // N_GENE

    def one_block(running, pieces):
        count_rows, coef_rows, shift_rows, load_rows = pieces
        observed = count_rows.astype(jnp.float32)
        linear = jnp.dot(jnp.concatenate([coef_rows, shift_rows], axis=1), stacked, precision=highest)
        latent = lax.dot_general(load_rows.astype(jnp.float32), factors.astype(jnp.float32), contract, preferred_element_type=jnp.float32)
        linear_pred = offset[None, :] + linear + latent
        expected = jnp.exp(linear_pred)
        weight = expected * live_mask
        residual = (observed - expected) * live_mask
        gram_part = lax.dot_general(weight, pairs, contract, precision=highest)
        score = lax.dot_general(residual, design, contract, precision=highest)
        beta_step = newton_solve(gram_part, score)
        expected_next = jnp.exp(linear_pred + jnp.dot(beta_step, design, precision=highest))
        weight_next = expected_next * live_mask
        residual_next = (observed - expected_next) * live_mask
        grad_load = jnp.dot(residual_next, factors_wide, precision=highest)
        curv_load = jnp.dot(weight_next, factors_wide * factors_wide, precision=highest)
        loads_wide = load_rows.astype(jnp.float32)
        back = (((0,), (0,)), ((), ()))
        grad_fact = running[0] + lax.dot_general(residual_next, loads_wide, back, precision=highest)
        curv_fact = running[1] + lax.dot_general(weight_next, loads_wide * loads_wide, back, precision=highest)
        return ((grad_fact, curv_fact), (beta_step, grad_load / jnp.sqrt(curv_load + 1.0)))
    pieces = (counts.reshape(N_GENE, gene_block, CELLS), coefficients.reshape(N_GENE, gene_block, columns), batch_effect.reshape(N_GENE, gene_block, BATCHES), loadings.reshape(N_GENE, gene_block, FACTORS))
    start = (jnp.zeros((CELLS, FACTORS), jnp.float32), jnp.zeros((CELLS, FACTORS), jnp.float32))
    sums, outputs = lax.scan(one_block, start, pieces)
    beta_step = outputs[0].reshape(GENES, columns)
    loading_score = outputs[1].reshape(GENES, FACTORS)
    factor_step = sums[0] / (sums[1] + 1.0)
    return (beta_step, factor_step, loading_score)
```

```python
import functools

import jax
import jax.numpy as jnp
from jax import lax
from jax.experimental import pallas as pl
from jax.experimental.pallas import tpu as pltpu
from jax.sharding import PartitionSpec as P

GENES = 3072
SPL = 16
BATCHES = 64


ridge_weight = 1.0


def design_rows(knot_bin, depth_frac, cell_covariates):
    levels = jnp.arange(SPL, dtype=jnp.int32)[:, None]
    fraction = depth_frac[None, :]
    hat_basis = jnp.where(levels == knot_bin[None, :], 1.0 - fraction, 0.0)
    hat_basis = hat_basis + jnp.where(levels == knot_bin[None, :] + 1, fraction, 0.0)
    return jnp.concatenate([hat_basis, cell_covariates], axis=0)


def newton_solve(gram_flat, score):
    columns = score.shape[-1]
    identity = jnp.eye(columns, dtype=gram_flat.dtype)
    system = gram_flat.reshape(-1, columns, columns) + ridge_weight * identity
    factor_lower = jnp.linalg.cholesky(system)
    middle = jax.scipy.linalg.solve_triangular(factor_lower, score[..., None], lower=True)
    return jax.scipy.linalg.solve_triangular(factor_lower, middle, lower=True, trans=1)[..., 0]


def local_plain(
    counts,
    batch_id,
    live_cells,
    knot_bin,
    depth_frac,
    cell_covariates,
    coefficients,
    batch_effect,
    factors,
    loadings,
):
    highest = lax.Precision.HIGHEST
    contract = (((1,), (1,)), ((), ()))
    observed = counts.astype(jnp.float32)
    totals = lax.psum(jnp.sum(observed, axis=0), "gene")
    offset = jnp.log((1.0 + totals) / GENES)
    slot_count = observed.shape[1]
    live_mask = (jnp.arange(slot_count, dtype=jnp.int32) < live_cells[0]).astype(jnp.float32)
    design = design_rows(knot_bin, depth_frac, cell_covariates)
    columns = design.shape[0]
    onehot = (jnp.arange(BATCHES, dtype=jnp.int32)[:, None] == batch_id[None, :]).astype(
        jnp.float32
    )
    stacked = jnp.concatenate([design, onehot], axis=0)
    linear = jnp.dot(
        jnp.concatenate([coefficients, batch_effect], axis=1), stacked, precision=highest
    )
    latent = lax.dot_general(loadings, factors, contract, preferred_element_type=jnp.float32)
    linear_pred = offset[None, :] + linear + latent
    expected = jnp.exp(linear_pred)
    weight = expected * live_mask
    residual = (observed - expected) * live_mask
    pairs = (design[:, None, :] * design[None, :, :]).reshape(columns * columns, slot_count)
    gram_part = lax.dot_general(weight, pairs, contract, precision=highest)
    score_part = lax.dot_general(residual, design, contract, precision=highest)
    gram_share, score_share = (
        lax.psum_scatter(gram_part, "cell", scatter_dimension=0, tiled=True),
        lax.psum_scatter(score_part, "cell", scatter_dimension=0, tiled=True),
    )
    step_share = newton_solve(gram_share, score_share)
    beta_step = lax.all_gather(step_share, "cell", axis=0, tiled=True)
    expected_next = jnp.exp(linear_pred + jnp.dot(beta_step, design, precision=highest))
    weight_next = expected_next * live_mask
    residual_next = (observed - expected_next) * live_mask
    factors_wide = factors.astype(jnp.float32)
    loads_wide = loadings.astype(jnp.float32)
    grad_load = jnp.dot(residual_next, factors_wide, precision=highest)
    curv_load = jnp.dot(weight_next, factors_wide * factors_wide, precision=highest)
    back = (((0,), (0,)), ((), ()))
    grad_fact = lax.dot_general(residual_next, loads_wide, back, precision=highest)
    curv_fact = lax.dot_general(weight_next, loads_wide * loads_wide, back, precision=highest)
    grad_load, curv_load = lax.psum((grad_load, curv_load), "cell")
    grad_fact, curv_fact = lax.psum((grad_fact, curv_fact), "gene")
    factor_step = grad_fact / (curv_fact + 1.0)
    loading_score = grad_load / jnp.sqrt(curv_load + 1.0)
    return (beta_step, factor_step, loading_score)


MESH = pl.DeviceIdType.MESH
F32, BF16 = jnp.float32, jnp.bfloat16
VM = pl.BlockSpec(memory_space=pltpu.VMEM)
ROWS_BY_ROWS = (((1,), (1,)), ((), ()))
ACROSS = (((1,), (0,)), ((), ()))
DOWN = (((0,), (0,)), ((), ()))
LIMIT = 60 * 1024 * 1024


def split(x):
    high = x.astype(BF16)
    return high, (x - high.astype(F32)).astype(BF16)


def mul(a, b, dims):
    return lax.dot_general(a, b, dims, preferred_element_type=F32)


def remote(src, dst, send, recv, where):
    return pltpu.make_async_remote_copy(
        src_ref=src, dst_ref=dst, send_sem=send, recv_sem=recv, device_id=where, device_id_type=MESH
    )


def meet(groups):
    barrier = pltpu.get_barrier_semaphore()
    count = 0
    for axis, n in groups:
        me = lax.axis_index(axis)
        for d in range(1, n):
            pl.semaphore_signal(
                barrier, inc=1, device_id={axis: lax.rem(me + d, n)}, device_id_type=MESH
            )
        count += n - 1
    pl.semaphore_wait(barrier, count)


def totals_kernel(n, x_ref, o_ref, recv, send_sem, recv_sem):
    me = lax.axis_index("gene")
    meet((("gene", n),))
    copies = []
    for d in range(1, n):
        copies.append(
            remote(
                x_ref, recv.at[d - 1], send_sem.at[d - 1], recv_sem.at[d - 1],
                {"gene": lax.rem(me + d, n)},
            )
        )
        copies[-1].start()
    total = x_ref[...]
    for d in range(1, n):
        copies[d - 1].wait()
        total = total + recv[d - 1]
    o_ref[...] = total


def design_of(knot_ref, frac_ref, cov_ref):
    slots = knot_ref.shape[1]
    levels = lax.broadcasted_iota(jnp.int32, (SPL, slots), 0)
    knot, frac = knot_ref[...], frac_ref[...]
    hats = jnp.where(levels == knot, 1.0 - frac, 0.0)
    hats = hats + jnp.where(levels == knot + 1, frac, 0.0)
    return hats, cov_ref[...]


def first_kernel(
    counts_ref, totals_ref, batch_ref, live_ref, knot_ref, frac_ref, cov_ref, coef_ref, shift_ref,
    factors_ref, loads_ref, g_ref, lin_ref, rhs, pair_hi, pair_lo, des_hi, des_lo, extra,
):
    slots = counts_ref.shape[1]

    @pl.when(pl.program_id(0) == 0)
    def _():
        hats, cov = design_of(knot_ref, frac_ref, cov_ref)
        ncov = cov.shape[0]
        half = ncov // 2
        design_hi, design_lo = split(jnp.concatenate([hats, cov], axis=0))
        hot = lax.broadcasted_iota(jnp.int32, (BATCHES, slots), 0) == batch_ref[...]
        hot = jnp.where(hot, 1.0, 0.0).astype(BF16)
        width = SPL + ncov
        rhs[0:width] = design_hi
        rhs[width : 2 * width] = design_hi
        rhs[2 * width : 3 * width] = design_lo
        rhs[3 * width : 3 * width + BATCHES] = hot
        rhs[3 * width + BATCHES : 3 * width + 2 * BATCHES] = hot

        def put(at, block):
            high, low = split(block)
            pair_hi[at : at + block.shape[0]] = high
            pair_lo[at : at + block.shape[0]] = low

        at = 0
        for p in range(SPL):
            put(at, hats[p : p + 1] * cov)
            at += ncov
        for i in range(half):
            put(at, cov[i : i + 1] * cov)
            at += ncov
        for i in range(half, ncov, 2):
            put(
                at,
                jnp.concatenate(
                    [cov[i : i + 1] * cov[half:], cov[i + 1 : i + 2] * cov[half:]], axis=0
                ),
            )
            at += ncov
        put(at, hats * hats)
        at += SPL
        later = jnp.concatenate([hats[1:], jnp.zeros((1, slots), F32)], axis=0)
        put(at, hats * later)
        at += SPL
        put(at, jnp.zeros((width, slots), F32))
        des_hi[...] = jnp.zeros(des_hi.shape, BF16)
        des_lo[...] = jnp.zeros(des_lo.shape, BF16)
        des_hi[128 - width : 128] = design_hi
        des_lo[128 - width : 128] = design_lo
        extra[0:1] = jnp.log((1.0 + totals_ref[...]) / GENES)
        places = lax.broadcasted_iota(jnp.int32, (1, slots), 1)
        extra[1:2] = jnp.where(places < live_ref[0], 1.0, 0.0)

    coef_hi, coef_lo = split(coef_ref[...])
    shift_hi, shift_lo = split(shift_ref[...])
    lhs = jnp.concatenate([coef_hi, coef_lo, coef_hi, shift_hi, shift_lo], axis=1)
    linear = mul(lhs, rhs[...], ACROSS) + mul(loads_ref[...], factors_ref[...], ROWS_BY_ROWS)
    linear = linear + extra[0:1]
    lin_ref[...] = linear
    mask = extra[1:2]
    expected = jnp.exp(linear)
    w_hi, w_lo = split(expected * mask)
    r_hi, r_lo = split((counts_ref[...].astype(F32) - expected) * mask)
    gram = mul(w_hi, pair_hi[...], ROWS_BY_ROWS)
    gram = gram + mul(w_hi, pair_lo[...], ROWS_BY_ROWS)
    gram = gram + mul(w_lo, pair_hi[...], ROWS_BY_ROWS)
    score = mul(r_hi, des_hi[...], ROWS_BY_ROWS)
    score = score + mul(r_hi, des_lo[...], ROWS_BY_ROWS)
    score = score + mul(r_lo, des_hi[...], ROWS_BY_ROWS)
    blocks, rows, wide = g_ref.shape
    g_ref[:, :, : wide - 128] = gram[:, : wide - 128].reshape(blocks, rows, wide - 128)
    g_ref[:, :, wide - 128 :] = (gram[:, wide - 128 :] + score).reshape(blocks, rows, 128)


def solve(g, x):
    half = SPL // 2
    cov_at, low_at, hat_at = SPL * SPL, SPL * SPL + half * SPL, SPL * SPL + half * SPL + half * half
    off_at, score_at = hat_at + SPL, hat_at + 2 * SPL
    spot = lax.broadcasted_iota(jnp.int32, (half, g.shape[1]), 0)

    def one(block, i):
        return block[i : i + 1]

    lo = {}
    hi = {}
    for i in range(SPL):
        unit = jnp.where(spot == i % half, ridge_weight, 0.0)
        if i < half:
            lo[i] = g[cov_at + i * SPL : cov_at + i * SPL + half] + unit
            hi[i] = g[cov_at + i * SPL + half : cov_at + (i + 1) * SPL]
        else:
            hi[i] = g[low_at + (i - half) * half : low_at + (i - half + 1) * half] + unit
    b_lo = g[score_at + SPL : score_at + SPL + half]
    b_hi = g[score_at + SPL + half : score_at + 2 * SPL]
    pivot_inv, edge, side_lo, side_hi, rest = [], [], [], [], []
    for p in range(SPL):
        d = g[hat_at + p : hat_at + p + 1] + ridge_weight
        u_lo = g[p * SPL : p * SPL + half]
        u_hi = g[p * SPL + half : (p + 1) * SPL]
        b = g[score_at + p : score_at + p + 1]
        if p > 0:
            ratio = edge[-1] * pivot_inv[-1]
            d = d - ratio * edge[-1]
            u_lo = u_lo - ratio * side_lo[-1]
            u_hi = u_hi - ratio * side_hi[-1]
            b = b - ratio * rest[-1]
        inv = 1.0 / d
        pivot_inv.append(inv)
        edge.append(g[off_at + p : off_at + p + 1])
        side_lo.append(u_lo)
        side_hi.append(u_hi)
        rest.append(b)
        scaled_lo, scaled_hi = u_lo * inv, u_hi * inv
        b_lo = b_lo - scaled_lo * b
        b_hi = b_hi - scaled_hi * b
        for i in range(SPL):
            if i < half:
                f = one(scaled_lo, i)
                lo[i] = lo[i] - f * u_lo
            else:
                f = one(scaled_hi, i - half)
            hi[i] = hi[i] - f * u_hi
    c_inv, c_rest = [], []
    for j in range(SPL):
        if j < half:
            inv = 1.0 / one(lo[j], j)
            b = one(b_lo, j)
            s_lo = lo[j] * inv
            b_lo = b_lo - s_lo * b
        else:
            inv = 1.0 / one(hi[j], j - half)
            b = one(b_hi, j - half)
        s_hi = hi[j] * inv
        b_hi = b_hi - s_hi * b
        c_inv.append(inv)
        c_rest.append(b)
        for i in range(j + 1, SPL):
            if i < half:
                f = one(s_lo, i)
                lo[i] = lo[i] - f * lo[j]
            else:
                f = one(s_hi, i - half)
            hi[i] = hi[i] - f * hi[j]
    for j in reversed(range(SPL)):
        found = c_rest[j] * c_inv[j]
        x[SPL + j : SPL + j + 1] = found
        for i in range(j):
            c_rest[i] = c_rest[i] - (one(hi[i], j - half) if j >= half else one(lo[i], j)) * found
    x_lo, x_hi = x[SPL : SPL + half], x[SPL + half : 2 * SPL]
    after = None
    for p in reversed(range(SPL)):
        gone = jnp.sum(side_lo[p] * x_lo + side_hi[p] * x_hi, axis=0, keepdims=True)
        b = rest[p] - gone
        if after is not None:
            b = b - edge[p] * after
        after = b * pivot_inv[p]
        x[p : p + 1] = after


def newton_kernel(
    n, g_ref, o_ref, from_pair, to_far, from_far, tall, turned, mine, theirs,
    pair_send, pair_recv, far_send, far_recv, out_send, out_recv,
):
    me = lax.axis_index("cell")
    core, chip = lax.rem(me, 2), me // 2
    chips, rows, wide = n // 2, g_ref.shape[1], g_ref.shape[2]
    meet((("cell", n),))
    pair = []
    for d in list(range(1, chips)) + [0]:
        k = lax.rem(chip + d, chips)
        pair.append(
            remote(
                g_ref.at[2 * k + 1 - core], from_pair.at[d], pair_send.at[d], pair_recv.at[d],
                {"cell": me + 1 - 2 * core},
            )
        )
        pair[-1].start()
    far = []
    for d in range(1, chips):
        k = lax.rem(chip + d, chips)
        pair[d - 1].wait()
        to_far[d - 1] = g_ref[2 * k + core] + from_pair[d]
        far.append(
            remote(
                to_far.at[d - 1], from_far.at[d - 1], far_send.at[d - 1], far_recv.at[d - 1],
                {"cell": 2 * k + core},
            )
        )
        far[-1].start()
    pair[chips - 1].wait()
    total = g_ref[me] + from_pair[0]
    for d in range(1, chips):
        far[d - 1].wait()
        total = total + from_far[d - 1]
    tall[0:rows] = total
    if rows < 128:
        tall[rows:128] = jnp.zeros((128 - rows, wide), F32)
    turned[...] = tall[...].T
    solve(turned, mine)
    out = []
    for d in range(1, n):
        out.append(
            remote(
                mine, theirs.at[d - 1], out_send.at[d - 1], out_recv.at[d - 1],
                {"cell": lax.rem(me + d, n)},
            )
        )
        out[-1].start()
    width = mine.shape[0]
    fill = jnp.zeros((128 - width, 128), F32)

    def put(owner, block):
        o_ref[owner] = jnp.concatenate([block, fill], axis=0).T[:rows, :width]

    put(me, mine[...])
    for d in range(1, n):
        out[d - 1].wait()
        put(lax.rem(me + n - d, n), theirs[d - 1])


def second_kernel(
    counts_ref, lin_ref, live_ref, knot_ref, frac_ref, cov_ref, beta_ref, factors_ref, loads_ref,
    gl_ref, gf_ref, rhs, mask_ref, f_one, f_hi, f_lo,
):
    slots = counts_ref.shape[1]
    step = pl.program_id(0)

    def spread(block):
        wide = block.astype(F32)
        zero = jnp.zeros(wide.shape, F32)
        square_hi, square_lo = split(jnp.concatenate([zero, wide * wide], axis=1))
        return jnp.concatenate([wide, zero], axis=1).astype(BF16), square_hi, square_lo

    @pl.when(step == 0)
    def _():
        hats, cov = design_of(knot_ref, frac_ref, cov_ref)
        design_hi, design_lo = split(jnp.concatenate([hats, cov], axis=0))
        width = design_hi.shape[0]
        rhs[0:width] = design_hi
        rhs[width : 2 * width] = design_hi
        rhs[2 * width : 3 * width] = design_lo
        places = lax.broadcasted_iota(jnp.int32, (1, slots), 1)
        mask_ref[0:1] = jnp.where(places < live_ref[0], 1.0, 0.0)
        f_one[...], f_hi[...], f_lo[...] = spread(factors_ref[...])
        gf_ref[...] = jnp.zeros(gf_ref.shape, F32)

    blocks, rows, width = beta_ref.shape
    beta_hi, beta_lo = split(beta_ref[...].reshape(blocks * rows, width))
    delta = mul(jnp.concatenate([beta_hi, beta_lo, beta_hi], axis=1), rhs[...], ACROSS)
    mask = mask_ref[0:1]
    expected = jnp.exp(lin_ref[...] + delta)
    w_hi, w_lo = split(expected * mask)
    r_hi, r_lo = split((counts_ref[...].astype(F32) - expected) * mask)
    gl = mul(r_hi, f_one[...], ACROSS) + mul(r_lo, f_one[...], ACROSS)
    gl = gl + mul(w_hi, f_hi[...], ACROSS)
    gl = gl + mul(w_hi, f_lo[...], ACROSS) + mul(w_lo, f_hi[...], ACROSS)
    gl_ref[...] = gl.reshape(gl_ref.shape)
    l_one, l_hi, l_lo = spread(loads_ref[...])
    gf = mul(l_one, r_hi, DOWN) + mul(l_one, r_lo, DOWN)
    gf = gf + mul(l_hi, w_hi, DOWN) + mul(l_lo, w_hi, DOWN) + mul(l_hi, w_lo, DOWN)
    span = gf_ref.shape[2]
    for j in range(gf_ref.shape[0]):
        gf_ref[j] += gf[:, j * span : (j + 1) * span]


def last_kernel(
    n, m, gl_ref, gf_ref, ls_ref, fs_ref, from_c, my_l, their_l, from_g, my_f, their_f,
    c_send, c_recv, g_send, g_recv, l_send, l_recv, f_send, f_recv,
):
    cell, gene = lax.axis_index("cell"), lax.axis_index("gene")
    half = gl_ref.shape[2] // 2
    span = gf_ref.shape[2]
    meet((("cell", n), ("gene", m)))
    across, along = [], []
    for d in range(1, m):
        to = lax.rem(gene + d, m)
        along.append(
            remote(gf_ref.at[to], from_g.at[d - 1], g_send.at[d - 1], g_recv.at[d - 1], {"gene": to})
        )
        along[-1].start()
    for d in range(1, n):
        to = lax.rem(cell + d, n)
        across.append(
            remote(gl_ref.at[to], from_c.at[d - 1], c_send.at[d - 1], c_recv.at[d - 1], {"cell": to})
        )
        across[-1].start()
    total = gl_ref[cell]
    for d in range(1, n):
        across[d - 1].wait()
        total = total + from_c[d - 1]
    my_l[...] = total[:, :half] / jnp.sqrt(total[:, half:] + 1.0)
    out_l, out_f = [], []
    for d in range(1, n):
        out_l.append(
            remote(
                my_l, their_l.at[d - 1], l_send.at[d - 1], l_recv.at[d - 1],
                {"cell": lax.rem(cell + d, n)},
            )
        )
        out_l[-1].start()
    total = gf_ref[gene]
    for d in range(1, m):
        along[d - 1].wait()
        total = total + from_g[d - 1]
    my_f[...] = total[:half] / (total[half:] + 1.0)
    for d in range(1, m):
        out_f.append(
            remote(
                my_f, their_f.at[d - 1], f_send.at[d - 1], f_recv.at[d - 1],
                {"gene": lax.rem(gene + d, m)},
            )
        )
        out_f[-1].start()
    ls_ref[cell] = my_l[...]
    for d in range(1, n):
        out_l[d - 1].wait()
        ls_ref[lax.rem(cell + n - d, n)] = their_l[d - 1]
    fill = jnp.zeros((half, span), F32)

    def put(owner, block):
        fs_ref[owner] = jnp.concatenate([block, fill], axis=0).T[:, :half]

    put(gene, my_f[...])
    for d in range(1, m):
        out_f[d - 1].wait()
        put(lax.rem(gene + m - d, m), their_f[d - 1])


def local_fused(
    n, m, counts, batch_id, live_cells, knot_bin, depth_frac, cell_covariates, coefficients,
    batch_effect, factors, loadings,
):
    genes, slots = counts.shape
    rows, span, latent = genes // n, slots // m, factors.shape[1]
    ncov = cell_covariates.shape[0]
    width = SPL + ncov
    wide = SPL * ncov + ncov * ncov * 3 // 4 + 2 * SPL + width
    steps = 2
    tile, blocks = genes // steps, n // steps
    dma = pltpu.SemaphoreType.DMA
    shape = jax.ShapeDtypeStruct

    def params(**kw):
        return pltpu.CompilerParams(vmem_limit_bytes=LIMIT, **kw)

    part = jnp.sum(counts, axis=0, keepdims=True).astype(F32)
    totals = pl.pallas_call(
        functools.partial(totals_kernel, m),
        out_shape=shape((1, slots), F32),
        in_specs=[VM],
        out_specs=VM,
        scratch_shapes=[pltpu.VMEM((m - 1, 1, slots), F32), dma((m - 1,)), dma((m - 1,))],
        compiler_params=params(collective_id=0, has_side_effects=True),
        name="totals",
    )(part)

    def by_rows(*tail):
        return pl.BlockSpec((tile,) + tail, lambda i: (i,) + (0,) * len(tail))

    def by_blocks(*tail):
        return pl.BlockSpec((blocks,) + tail, lambda i: (i,) + (0,) * len(tail))

    def whole(*dims):
        return pl.BlockSpec(dims, lambda i: (0,) * len(dims))

    smem = pl.BlockSpec(memory_space=pltpu.SMEM)
    knot, frac, batch = (v.reshape(1, slots) for v in (knot_bin, depth_frac, batch_id))
    line = whole(1, slots)
    gram, lin = pl.pallas_call(
        first_kernel,
        grid=(steps,),
        out_shape=(shape((n, rows, wide), F32), shape((genes, slots), F32)),
        in_specs=[
            by_rows(slots), line, line, smem, line, line, whole(ncov, slots),
            by_rows(width), by_rows(BATCHES), whole(slots, latent), by_rows(latent),
        ],
        out_specs=(by_blocks(rows, wide), by_rows(slots)),
        scratch_shapes=[
            pltpu.VMEM((3 * width + 2 * BATCHES, slots), BF16),
            pltpu.VMEM((wide, slots), BF16),
            pltpu.VMEM((wide, slots), BF16),
            pltpu.VMEM((128, slots), BF16),
            pltpu.VMEM((128, slots), BF16),
            pltpu.VMEM((8, slots), F32),
        ],
        compiler_params=params(),
        name="first",
    )(
        counts, totals, batch, live_cells, knot, frac, cell_covariates, coefficients,
        batch_effect, factors, loadings,
    )
    chips = n // 2
    beta = pl.pallas_call(
        functools.partial(newton_kernel, n),
        out_shape=shape((n, rows, width), F32),
        in_specs=[VM],
        out_specs=VM,
        scratch_shapes=[
            pltpu.VMEM((chips, rows, wide), F32),
            pltpu.VMEM((chips - 1, rows, wide), F32),
            pltpu.VMEM((chips - 1, rows, wide), F32),
            pltpu.VMEM((128, wide), F32),
            pltpu.VMEM((wide, 128), F32),
            pltpu.VMEM((width, 128), F32),
            pltpu.VMEM((n - 1, width, 128), F32),
            dma((chips,)), dma((chips,)), dma((chips - 1,)), dma((chips - 1,)),
            dma((n - 1,)), dma((n - 1,)),
        ],
        compiler_params=params(collective_id=1, has_side_effects=True),
        name="newton",
    )(gram)
    gl, gf = pl.pallas_call(
        second_kernel,
        grid=(steps,),
        out_shape=(shape((n, rows, 2 * latent), F32), shape((m, 2 * latent, span), F32)),
        in_specs=[
            by_rows(slots), by_rows(slots), smem, line, line, whole(ncov, slots),
            by_blocks(rows, width), whole(slots, latent), by_rows(latent),
        ],
        out_specs=(by_blocks(rows, 2 * latent), whole(m, 2 * latent, span)),
        scratch_shapes=[
            pltpu.VMEM((3 * width, slots), BF16),
            pltpu.VMEM((8, slots), F32),
            pltpu.VMEM((slots, 2 * latent), BF16),
            pltpu.VMEM((slots, 2 * latent), BF16),
            pltpu.VMEM((slots, 2 * latent), BF16),
        ],
        compiler_params=params(),
        name="second",
    )(counts, lin, live_cells, knot, frac, cell_covariates, beta, factors, loadings)
    ls, fs = pl.pallas_call(
        functools.partial(last_kernel, n, m),
        out_shape=(shape((n, rows, latent), F32), shape((m, span, latent), F32)),
        in_specs=[VM, VM],
        out_specs=(VM, VM),
        scratch_shapes=[
            pltpu.VMEM((n - 1, rows, 2 * latent), F32),
            pltpu.VMEM((rows, latent), F32),
            pltpu.VMEM((n - 1, rows, latent), F32),
            pltpu.VMEM((m - 1, 2 * latent, span), F32),
            pltpu.VMEM((latent, span), F32),
            pltpu.VMEM((m - 1, latent, span), F32),
            dma((n - 1,)), dma((n - 1,)), dma((m - 1,)), dma((m - 1,)),
            dma((n - 1,)), dma((n - 1,)), dma((m - 1,)), dma((m - 1,)),
        ],
        compiler_params=params(collective_id=2, has_side_effects=True),
        name="last",
    )(gl, gf)
    return beta.reshape(genes, width), fs.reshape(slots, latent), ls.reshape(genes, latent)


def local(n, m, *args):
    counts, cov, factors = args[0], args[5], args[8]
    genes, slots = counts.shape
    fits = (
        n % 2 == 0
        and n > 2
        and m > 1
        and genes % (16 * n) == 0
        and genes // n <= 128
        and slots % (128 * m) == 0
        and cov.shape[0] == SPL
        and factors.shape[1] == 64
    )
    if fits:
        return local_fused(n, m, *args)
    return local_plain(*args)


def solution(mesh):
    placed = (
        P("gene", "cell"),
        P("cell"),
        P("cell"),
        P("cell"),
        P("cell"),
        P(None, "cell"),
        P("gene", None),
        P("gene", None),
        P("cell", None),
        P("gene", None),
    )
    return jax.shard_map(
        functools.partial(local, mesh.shape["cell"], mesh.shape["gene"]),
        mesh=mesh,
        in_specs=placed,
        out_specs=(P("gene", None), P("cell", None), P("gene", None)),
        check_vma=False,
    )
```

```python
import functools

import jax
import jax.numpy as jnp
from jax import lax
from jax.experimental import pallas as pl
from jax.experimental.pallas import tpu as pltpu
from jax.sharding import PartitionSpec as P

GENES = 3072
SPL = 16
BATCHES = 64


ridge_weight = 1.0


def design_rows(knot_bin, depth_frac, cell_covariates):
    levels = jnp.arange(SPL, dtype=jnp.int32)[:, None]
    fraction = depth_frac[None, :]
    hat_basis = jnp.where(levels == knot_bin[None, :], 1.0 - fraction, 0.0)
    hat_basis = hat_basis + jnp.where(levels == knot_bin[None, :] + 1, fraction, 0.0)
    return jnp.concatenate([hat_basis, cell_covariates], axis=0)


def newton_solve(gram_flat, score):
    columns = score.shape[-1]
    identity = jnp.eye(columns, dtype=gram_flat.dtype)
    system = gram_flat.reshape(-1, columns, columns) + ridge_weight * identity
    factor_lower = jnp.linalg.cholesky(system)
    middle = jax.scipy.linalg.solve_triangular(factor_lower, score[..., None], lower=True)
    return jax.scipy.linalg.solve_triangular(factor_lower, middle, lower=True, trans=1)[..., 0]


def local_plain(
    counts,
    batch_id,
    live_cells,
    knot_bin,
    depth_frac,
    cell_covariates,
    coefficients,
    batch_effect,
    factors,
    loadings,
):
    highest = lax.Precision.HIGHEST
    contract = (((1,), (1,)), ((), ()))
    observed = counts.astype(jnp.float32)
    totals = lax.psum(jnp.sum(observed, axis=0), "gene")
    offset = jnp.log((1.0 + totals) / GENES)
    slot_count = observed.shape[1]
    live_mask = (jnp.arange(slot_count, dtype=jnp.int32) < live_cells[0]).astype(jnp.float32)
    design = design_rows(knot_bin, depth_frac, cell_covariates)
    columns = design.shape[0]
    onehot = (jnp.arange(BATCHES, dtype=jnp.int32)[:, None] == batch_id[None, :]).astype(
        jnp.float32
    )
    stacked = jnp.concatenate([design, onehot], axis=0)
    linear = jnp.dot(
        jnp.concatenate([coefficients, batch_effect], axis=1), stacked, precision=highest
    )
    latent = lax.dot_general(loadings, factors, contract, preferred_element_type=jnp.float32)
    linear_pred = offset[None, :] + linear + latent
    expected = jnp.exp(linear_pred)
    weight = expected * live_mask
    residual = (observed - expected) * live_mask
    pairs = (design[:, None, :] * design[None, :, :]).reshape(columns * columns, slot_count)
    gram_part = lax.dot_general(weight, pairs, contract, precision=highest)
    score_part = lax.dot_general(residual, design, contract, precision=highest)
    gram_share, score_share = (
        lax.psum_scatter(gram_part, "cell", scatter_dimension=0, tiled=True),
        lax.psum_scatter(score_part, "cell", scatter_dimension=0, tiled=True),
    )
    step_share = newton_solve(gram_share, score_share)
    beta_step = lax.all_gather(step_share, "cell", axis=0, tiled=True)
    expected_next = jnp.exp(linear_pred + jnp.dot(beta_step, design, precision=highest))
    weight_next = expected_next * live_mask
    residual_next = (observed - expected_next) * live_mask
    factors_wide = factors.astype(jnp.float32)
    loads_wide = loadings.astype(jnp.float32)
    grad_load = jnp.dot(residual_next, factors_wide, precision=highest)
    curv_load = jnp.dot(weight_next, factors_wide * factors_wide, precision=highest)
    back = (((0,), (0,)), ((), ()))
    grad_fact = lax.dot_general(residual_next, loads_wide, back, precision=highest)
    curv_fact = lax.dot_general(weight_next, loads_wide * loads_wide, back, precision=highest)
    grad_load, curv_load = lax.psum((grad_load, curv_load), "cell")
    grad_fact, curv_fact = lax.psum((grad_fact, curv_fact), "gene")
    factor_step = grad_fact / (curv_fact + 1.0)
    loading_score = grad_load / jnp.sqrt(curv_load + 1.0)
    return (beta_step, factor_step, loading_score)


MESH = pl.DeviceIdType.MESH
F32, BF16 = jnp.float32, jnp.bfloat16
VM = pl.BlockSpec(memory_space=pltpu.VMEM)
ROWS_BY_ROWS = (((1,), (1,)), ((), ()))
ACROSS = (((1,), (0,)), ((), ()))
DOWN = (((0,), (0,)), ((), ()))
LIMIT = 60 * 1024 * 1024


def split(x):
    high = x.astype(BF16)
    return high, (x - high.astype(F32)).astype(BF16)


def mul(a, b, dims):
    return lax.dot_general(a, b, dims, preferred_element_type=F32)


def remote(src, dst, send, recv, where):
    return pltpu.make_async_remote_copy(
        src_ref=src, dst_ref=dst, send_sem=send, recv_sem=recv, device_id=where, device_id_type=MESH
    )


def meet(groups):
    barrier = pltpu.get_barrier_semaphore()
    count = 0
    for axis, n in groups:
        me = lax.axis_index(axis)
        for d in range(1, n):
            pl.semaphore_signal(
                barrier, inc=1, device_id={axis: lax.rem(me + d, n)}, device_id_type=MESH
            )
        count += n - 1
    pl.semaphore_wait(barrier, count)


def totals_kernel(n, x_ref, o_ref, recv, send_sem, recv_sem):
    me = lax.axis_index("gene")
    meet((("gene", n),))
    copies = []
    for d in range(1, n):
        copies.append(
            remote(
                x_ref, recv.at[d - 1], send_sem.at[d - 1], recv_sem.at[d - 1],
                {"gene": lax.rem(me + d, n)},
            )
        )
        copies[-1].start()
    total = x_ref[...]
    for d in range(1, n):
        copies[d - 1].wait()
        total = total + recv[d - 1]
    o_ref[...] = total


def design_of(knot_ref, frac_ref, cov_ref):
    slots = knot_ref.shape[1]
    levels = lax.broadcasted_iota(jnp.int32, (SPL, slots), 0)
    knot, frac = knot_ref[...], frac_ref[...]
    hats = jnp.where(levels == knot, 1.0 - frac, 0.0)
    hats = hats + jnp.where(levels == knot + 1, frac, 0.0)
    return hats, cov_ref[...]


def first_kernel(
    counts_ref, totals_ref, batch_ref, live_ref, knot_ref, frac_ref, cov_ref, coef_ref, shift_ref,
    factors_ref, loads_ref, g_ref, lin_ref, rhs, pair_hi, pair_lo, des_hi, des_lo, extra,
):
    slots = counts_ref.shape[1]

    @pl.when(pl.program_id(0) == 0)
    def _():
        hats, cov = design_of(knot_ref, frac_ref, cov_ref)
        ncov = cov.shape[0]
        half = ncov // 2
        design_hi, design_lo = split(jnp.concatenate([hats, cov], axis=0))
        hot = lax.broadcasted_iota(jnp.int32, (BATCHES, slots), 0) == batch_ref[...]
        hot = jnp.where(hot, 1.0, 0.0).astype(BF16)
        width = SPL + ncov
        rhs[0:width] = design_hi
        rhs[width : 2 * width] = design_hi
        rhs[2 * width : 3 * width] = design_lo
        rhs[3 * width : 3 * width + BATCHES] = hot
        rhs[3 * width + BATCHES : 3 * width + 2 * BATCHES] = hot
        rhs[3 * width + 2 * BATCHES :] = factors_ref[...]

        def put(at, block):
            high, low = split(block)
            pair_hi[at : at + block.shape[0]] = high
            pair_lo[at : at + block.shape[0]] = low

        at = 0
        for p in range(SPL):
            put(at, hats[p : p + 1] * cov)
            at += ncov
        for i in range(half):
            put(at, cov[i : i + 1] * cov)
            at += ncov
        for i in range(half, ncov, 2):
            put(
                at,
                jnp.concatenate(
                    [cov[i : i + 1] * cov[half:], cov[i + 1 : i + 2] * cov[half:]], axis=0
                ),
            )
            at += ncov
        put(at, hats * hats)
        at += SPL
        later = jnp.concatenate([hats[1:], jnp.zeros((1, slots), F32)], axis=0)
        put(at, hats * later)
        at += SPL
        put(at, jnp.zeros((width, slots), F32))
        des_hi[...] = jnp.zeros(des_hi.shape, BF16)
        des_lo[...] = jnp.zeros(des_lo.shape, BF16)
        des_hi[128 - width : 128] = design_hi
        des_lo[128 - width : 128] = design_lo
        extra[0:1] = jnp.log((1.0 + totals_ref[...]) / GENES)
        places = lax.broadcasted_iota(jnp.int32, (1, slots), 1)
        extra[1:2] = jnp.where(places < live_ref[0], 1.0, 0.0)

    coef_hi, coef_lo = split(coef_ref[...])
    shift_hi, shift_lo = split(shift_ref[...])
    lhs = jnp.concatenate([coef_hi, coef_lo, coef_hi, shift_hi, shift_lo, loads_ref[...]], axis=0)
    linear = mul(lhs, rhs[...], DOWN) + extra[0:1]
    lin_ref[...] = linear
    mask = extra[1:2]
    expected = jnp.exp(linear)
    w_hi, w_lo = split(expected * mask)
    r_hi, r_lo = split((counts_ref[...].astype(F32) - expected) * mask)
    gram = mul(w_hi, pair_hi[...], ROWS_BY_ROWS)
    gram = gram + mul(w_hi, pair_lo[...], ROWS_BY_ROWS)
    gram = gram + mul(w_lo, pair_hi[...], ROWS_BY_ROWS)
    score = mul(r_hi, des_hi[...], ROWS_BY_ROWS)
    score = score + mul(r_hi, des_lo[...], ROWS_BY_ROWS)
    score = score + mul(r_lo, des_hi[...], ROWS_BY_ROWS)
    blocks, rows, wide = g_ref.shape
    g_ref[:, :, : wide - 128] = gram[:, : wide - 128].reshape(blocks, rows, wide - 128)
    g_ref[:, :, wide - 128 :] = (gram[:, wide - 128 :] + score).reshape(blocks, rows, 128)


def solve(g, x):
    half = SPL // 2
    cov_at, low_at, hat_at = SPL * SPL, SPL * SPL + half * SPL, SPL * SPL + half * SPL + half * half
    off_at, score_at = hat_at + SPL, hat_at + 2 * SPL
    spot = lax.broadcasted_iota(jnp.int32, (half, g.shape[1]), 0)

    def one(block, i):
        return block[i : i + 1]

    lo = {}
    hi = {}
    for i in range(SPL):
        unit = jnp.where(spot == i % half, ridge_weight, 0.0)
        if i < half:
            lo[i] = g[cov_at + i * SPL : cov_at + i * SPL + half] + unit
            hi[i] = g[cov_at + i * SPL + half : cov_at + (i + 1) * SPL]
        else:
            hi[i] = g[low_at + (i - half) * half : low_at + (i - half + 1) * half] + unit
    b_lo = g[score_at + SPL : score_at + SPL + half]
    b_hi = g[score_at + SPL + half : score_at + 2 * SPL]
    pivot_inv, edge, side_lo, side_hi, rest = [], [], [], [], []
    for p in range(SPL):
        d = g[hat_at + p : hat_at + p + 1] + ridge_weight
        u_lo = g[p * SPL : p * SPL + half]
        u_hi = g[p * SPL + half : (p + 1) * SPL]
        b = g[score_at + p : score_at + p + 1]
        if p > 0:
            ratio = edge[-1] * pivot_inv[-1]
            d = d - ratio * edge[-1]
            u_lo = u_lo - ratio * side_lo[-1]
            u_hi = u_hi - ratio * side_hi[-1]
            b = b - ratio * rest[-1]
        inv = 1.0 / d
        pivot_inv.append(inv)
        edge.append(g[off_at + p : off_at + p + 1])
        side_lo.append(u_lo)
        side_hi.append(u_hi)
        rest.append(b)
        scaled_lo, scaled_hi = u_lo * inv, u_hi * inv
        b_lo = b_lo - scaled_lo * b
        b_hi = b_hi - scaled_hi * b
        for i in range(SPL):
            if i < half:
                f = one(scaled_lo, i)
                lo[i] = lo[i] - f * u_lo
            else:
                f = one(scaled_hi, i - half)
            hi[i] = hi[i] - f * u_hi
    c_inv, c_rest = [], []
    for j in range(SPL):
        if j < half:
            inv = 1.0 / one(lo[j], j)
            b = one(b_lo, j)
            s_lo = lo[j] * inv
            b_lo = b_lo - s_lo * b
        else:
            inv = 1.0 / one(hi[j], j - half)
            b = one(b_hi, j - half)
        s_hi = hi[j] * inv
        b_hi = b_hi - s_hi * b
        c_inv.append(inv)
        c_rest.append(b)
        for i in range(j + 1, SPL):
            if i < half:
                f = one(s_lo, i)
                lo[i] = lo[i] - f * lo[j]
            else:
                f = one(s_hi, i - half)
            hi[i] = hi[i] - f * hi[j]
    for j in reversed(range(SPL)):
        found = c_rest[j] * c_inv[j]
        x[SPL + j : SPL + j + 1] = found
        for i in range(j):
            c_rest[i] = c_rest[i] - (one(hi[i], j - half) if j >= half else one(lo[i], j)) * found
    x_lo, x_hi = x[SPL : SPL + half], x[SPL + half : 2 * SPL]
    after = None
    for p in reversed(range(SPL)):
        gone = jnp.sum(side_lo[p] * x_lo + side_hi[p] * x_hi, axis=0, keepdims=True)
        b = rest[p] - gone
        if after is not None:
            b = b - edge[p] * after
        after = b * pivot_inv[p]
        x[p : p + 1] = after


def newton_kernel(
    n, g_ref, o_ref, from_pair, to_far, from_far, tall, turned, mine, theirs,
    pair_send, pair_recv, far_send, far_recv, out_send, out_recv,
):
    me = lax.axis_index("cell")
    core, chip = lax.rem(me, 2), me // 2
    chips, rows, wide = n // 2, g_ref.shape[1], g_ref.shape[2]
    meet((("cell", n),))
    pair = []
    for d in list(range(1, chips)) + [0]:
        k = lax.rem(chip + d, chips)
        pair.append(
            remote(
                g_ref.at[2 * k + 1 - core], from_pair.at[d], pair_send.at[d], pair_recv.at[d],
                {"cell": me + 1 - 2 * core},
            )
        )
        pair[-1].start()
    far = []
    for d in range(1, chips):
        k = lax.rem(chip + d, chips)
        pair[d - 1].wait()
        to_far[d - 1] = g_ref[2 * k + core] + from_pair[d]
        far.append(
            remote(
                to_far.at[d - 1], from_far.at[d - 1], far_send.at[d - 1], far_recv.at[d - 1],
                {"cell": 2 * k + core},
            )
        )
        far[-1].start()
    pair[chips - 1].wait()
    total = g_ref[me] + from_pair[0]
    for d in range(1, chips):
        far[d - 1].wait()
        total = total + from_far[d - 1]
    tall[0:rows] = total
    if rows < 128:
        tall[rows:128] = jnp.zeros((128 - rows, wide), F32)
    turned[...] = tall[...].T
    solve(turned, mine)
    out = []
    for d in range(1, n):
        out.append(
            remote(
                mine, theirs.at[d - 1], out_send.at[d - 1], out_recv.at[d - 1],
                {"cell": lax.rem(me + d, n)},
            )
        )
        out[-1].start()
    width = mine.shape[0]
    fill = jnp.zeros((128 - width, 128), F32)

    def put(owner, block):
        o_ref[owner] = jnp.concatenate([block, fill], axis=0).T[:rows, :width]

    put(me, mine[...])
    for d in range(1, n):
        out[d - 1].wait()
        put(lax.rem(me + n - d, n), theirs[d - 1])


def second_kernel(
    counts_ref, lin_ref, live_ref, knot_ref, frac_ref, cov_ref, beta_ref, factors_ref, loads_ref,
    gl_ref, gf_ref, turned_ref, rhs, mask_ref, f_one, f_hi, f_lo,
):
    slots = counts_ref.shape[1]
    step = pl.program_id(0)

    def spread(block):
        wide = block.astype(F32)
        zero = jnp.zeros(wide.shape, F32)
        square_hi, square_lo = split(jnp.concatenate([zero, wide * wide], axis=0))
        return jnp.concatenate([wide, zero], axis=0).astype(BF16), square_hi, square_lo

    @pl.when(step == 0)
    def _():
        hats, cov = design_of(knot_ref, frac_ref, cov_ref)
        design_hi, design_lo = split(jnp.concatenate([hats, cov], axis=0))
        width = design_hi.shape[0]
        rhs[0:width] = design_hi
        rhs[width : 2 * width] = design_hi
        rhs[2 * width : 3 * width] = design_lo
        places = lax.broadcasted_iota(jnp.int32, (1, slots), 1)
        mask_ref[0:1] = jnp.where(places < live_ref[0], 1.0, 0.0)
        f_one[...], f_hi[...], f_lo[...] = spread(factors_ref[...])
        gf_ref[...] = jnp.zeros(gf_ref.shape, F32)

    blocks, rows, width = beta_ref.shape
    beta = beta_ref[...].reshape(blocks * rows, width)
    beta_hi, beta_lo = split(beta)
    fill = jnp.zeros((blocks * rows, 128 - width), F32)
    turned_ref[...] = jnp.concatenate([beta, fill], axis=1).T[:width]
    delta = mul(jnp.concatenate([beta_hi, beta_lo, beta_hi], axis=1), rhs[...], ACROSS)
    mask = mask_ref[0:1]
    expected = jnp.exp(lin_ref[...] + delta)
    w_hi, w_lo = split(expected * mask)
    r_hi, r_lo = split((counts_ref[...].astype(F32) - expected) * mask)
    gl = mul(r_hi, f_one[...], ROWS_BY_ROWS) + mul(r_lo, f_one[...], ROWS_BY_ROWS)
    gl = gl + mul(w_hi, f_hi[...], ROWS_BY_ROWS)
    gl = gl + mul(w_hi, f_lo[...], ROWS_BY_ROWS) + mul(w_lo, f_hi[...], ROWS_BY_ROWS)
    gl_ref[...] = gl.reshape(gl_ref.shape)
    l_one, l_hi, l_lo = spread(loads_ref[...])
    gf = mul(l_one, r_hi, ACROSS) + mul(l_one, r_lo, ACROSS)
    gf = gf + mul(l_hi, w_hi, ACROSS) + mul(l_lo, w_hi, ACROSS) + mul(l_hi, w_lo, ACROSS)
    span = gf_ref.shape[2]
    for j in range(gf_ref.shape[0]):
        gf_ref[j] += gf[:, j * span : (j + 1) * span]


def last_kernel(
    n, m, gl_ref, gf_ref, ls_ref, fs_ref, from_c, my_l, their_l, from_g, my_f, their_f,
    c_send, c_recv, g_send, g_recv, l_send, l_recv, f_send, f_recv,
):
    cell, gene = lax.axis_index("cell"), lax.axis_index("gene")
    half = gl_ref.shape[2] // 2
    span = gf_ref.shape[2]
    meet((("cell", n), ("gene", m)))
    across, along = [], []
    for d in range(1, m):
        to = lax.rem(gene + d, m)
        along.append(
            remote(gf_ref.at[to], from_g.at[d - 1], g_send.at[d - 1], g_recv.at[d - 1], {"gene": to})
        )
        along[-1].start()
    for d in range(1, n):
        to = lax.rem(cell + d, n)
        across.append(
            remote(gl_ref.at[to], from_c.at[d - 1], c_send.at[d - 1], c_recv.at[d - 1], {"cell": to})
        )
        across[-1].start()
    total = gl_ref[cell]
    for d in range(1, n):
        across[d - 1].wait()
        total = total + from_c[d - 1]
    my_l[...] = total[:, :half] / jnp.sqrt(total[:, half:] + 1.0)
    their_l[cell] = my_l[...]
    out_l, out_f = [], []
    for d in range(1, n):
        out_l.append(
            remote(
                my_l, their_l.at[cell], l_send.at[d - 1], l_recv.at[d - 1],
                {"cell": lax.rem(cell + d, n)},
            )
        )
        out_l[-1].start()
    total = gf_ref[gene]
    for d in range(1, m):
        along[d - 1].wait()
        total = total + from_g[d - 1]
    my_f[...] = total[:half] / (total[half:] + 1.0)
    for d in range(1, m):
        out_f.append(
            remote(
                my_f, their_f.at[d - 1], f_send.at[d - 1], f_recv.at[d - 1],
                {"gene": lax.rem(gene + d, m)},
            )
        )
        out_f[-1].start()
    def put(owner, block):
        fs_ref[:, pl.ds(pl.multiple_of(owner * span, span), span)] = block

    put(gene, my_f[...])
    for d in range(1, n):
        out_l[d - 1].wait()
    found = their_l[...].reshape(ls_ref.shape[1], half)
    ls_ref[...] = jnp.concatenate([found, jnp.zeros(found.shape, F32)], axis=1).T[:half]
    for d in range(1, m):
        out_f[d - 1].wait()
        put(lax.rem(gene + m - d, m), their_f[d - 1])


def local_fused(
    n, m, counts, batch_id, live_cells, knot_bin, depth_frac, cell_covariates, coefficients,
    batch_effect, factors, loadings,
):
    genes, slots = counts.shape
    rows, span, latent = genes // n, slots // m, factors.shape[1]
    ncov = cell_covariates.shape[0]
    width = SPL + ncov
    wide = SPL * ncov + ncov * ncov * 3 // 4 + 2 * SPL + width
    steps = 2
    tile, blocks = genes // steps, n // steps
    dma = pltpu.SemaphoreType.DMA
    shape = jax.ShapeDtypeStruct

    def params(**kw):
        return pltpu.CompilerParams(vmem_limit_bytes=LIMIT, **kw)

    part = jnp.sum(counts, axis=0, keepdims=True).astype(F32)
    totals = pl.pallas_call(
        functools.partial(totals_kernel, m),
        out_shape=shape((1, slots), F32),
        in_specs=[VM],
        out_specs=VM,
        scratch_shapes=[pltpu.VMEM((m - 1, 1, slots), F32), dma((m - 1,)), dma((m - 1,))],
        compiler_params=params(collective_id=0, has_side_effects=True),
        name="totals",
    )(part)

    def by_rows(*tail):
        return pl.BlockSpec((tile,) + tail, lambda i: (i,) + (0,) * len(tail))

    def by_lanes(count):
        return pl.BlockSpec((count, tile), lambda i: (0, i))

    def by_blocks(*tail):
        return pl.BlockSpec((blocks,) + tail, lambda i: (i,) + (0,) * len(tail))

    def whole(*dims):
        return pl.BlockSpec(dims, lambda i: (0,) * len(dims))

    smem = pl.BlockSpec(memory_space=pltpu.SMEM)
    knot, frac, batch = (v.reshape(1, slots) for v in (knot_bin, depth_frac, batch_id))
    line = whole(1, slots)
    gram, lin = pl.pallas_call(
        first_kernel,
        grid=(steps,),
        out_shape=(shape((n, rows, wide), F32), shape((genes, slots), F32)),
        in_specs=[
            by_rows(slots), line, line, smem, line, line, whole(ncov, slots),
            by_lanes(width), by_lanes(BATCHES), whole(latent, slots), by_lanes(latent),
        ],
        out_specs=(by_blocks(rows, wide), by_rows(slots)),
        scratch_shapes=[
            pltpu.VMEM((3 * width + 2 * BATCHES + latent, slots), BF16),
            pltpu.VMEM((wide, slots), BF16),
            pltpu.VMEM((wide, slots), BF16),
            pltpu.VMEM((128, slots), BF16),
            pltpu.VMEM((128, slots), BF16),
            pltpu.VMEM((8, slots), F32),
        ],
        compiler_params=params(),
        name="first",
    )(
        counts, totals, batch, live_cells, knot, frac, cell_covariates, coefficients.T,
        batch_effect.T, factors.T, loadings.T,
    )
    chips = n // 2
    beta = pl.pallas_call(
        functools.partial(newton_kernel, n),
        out_shape=shape((n, rows, width), F32),
        in_specs=[VM],
        out_specs=VM,
        scratch_shapes=[
            pltpu.VMEM((chips, rows, wide), F32),
            pltpu.VMEM((chips - 1, rows, wide), F32),
            pltpu.VMEM((chips - 1, rows, wide), F32),
            pltpu.VMEM((128, wide), F32),
            pltpu.VMEM((wide, 128), F32),
            pltpu.VMEM((width, 128), F32),
            pltpu.VMEM((n - 1, width, 128), F32),
            dma((chips,)), dma((chips,)), dma((chips - 1,)), dma((chips - 1,)),
            dma((n - 1,)), dma((n - 1,)),
        ],
        compiler_params=params(collective_id=1, has_side_effects=True),
        name="newton",
    )(gram)
    gl, gf, beta_turned = pl.pallas_call(
        second_kernel,
        grid=(steps,),
        out_shape=(shape((n, rows, 2 * latent), F32), shape((m, 2 * latent, span), F32),
                   shape((width, genes), F32)),
        in_specs=[
            by_rows(slots), by_rows(slots), smem, line, line, whole(ncov, slots),
            by_blocks(rows, width), whole(latent, slots), by_lanes(latent),
        ],
        out_specs=(by_blocks(rows, 2 * latent), whole(m, 2 * latent, span), by_lanes(width)),
        scratch_shapes=[
            pltpu.VMEM((3 * width, slots), BF16),
            pltpu.VMEM((8, slots), F32),
            pltpu.VMEM((2 * latent, slots), BF16),
            pltpu.VMEM((2 * latent, slots), BF16),
            pltpu.VMEM((2 * latent, slots), BF16),
        ],
        compiler_params=params(),
        name="second",
    )(counts, lin, live_cells, knot, frac, cell_covariates, beta, factors.T, loadings.T)
    ls, fs = pl.pallas_call(
        functools.partial(last_kernel, n, m),
        out_shape=(shape((latent, genes), F32), shape((latent, slots), F32)),
        in_specs=[VM, VM],
        out_specs=(VM, VM),
        scratch_shapes=[
            pltpu.VMEM((n - 1, rows, 2 * latent), F32),
            pltpu.VMEM((rows, latent), F32),
            pltpu.VMEM((n, rows, latent), F32),
            pltpu.VMEM((m - 1, 2 * latent, span), F32),
            pltpu.VMEM((latent, span), F32),
            pltpu.VMEM((m - 1, latent, span), F32),
            dma((n - 1,)), dma((n - 1,)), dma((m - 1,)), dma((m - 1,)),
            dma((n - 1,)), dma((n - 1,)), dma((m - 1,)), dma((m - 1,)),
        ],
        compiler_params=params(collective_id=2, has_side_effects=True),
        name="last",
    )(gl, gf)
    return beta_turned.T, fs.T, ls.T


def local(n, m, *args):
    counts, cov, factors = args[0], args[5], args[8]
    genes, slots = counts.shape
    fits = (
        n % 2 == 0
        and n > 2
        and m > 1
        and genes % (16 * n) == 0
        and genes // n <= 128
        and slots % (128 * m) == 0
        and cov.shape[0] == SPL
        and factors.shape[1] == 64
    )
    if fits:
        return local_fused(n, m, *args)
    return local_plain(*args)


def solution(mesh):
    placed = (
        P("gene", "cell"),
        P("cell"),
        P("cell"),
        P("cell"),
        P("cell"),
        P(None, "cell"),
        P("gene", None),
        P("gene", None),
        P("cell", None),
        P("gene", None),
    )
    return jax.shard_map(
        functools.partial(local, mesh.shape["cell"], mesh.shape["gene"]),
        mesh=mesh,
        in_specs=placed,
        out_specs=(P("gene", None), P("cell", None), P("gene", None)),
        check_vma=False,
    )
```

```python
import functools

import jax
import jax.numpy as jnp
from jax import lax
from jax.experimental import pallas as pl
from jax.experimental.pallas import tpu as pltpu
from jax.sharding import PartitionSpec as P

GENES = 3072
SPL = 16
BATCHES = 64


ridge_weight = 1.0


def design_rows(knot_bin, depth_frac, cell_covariates):
    levels = jnp.arange(SPL, dtype=jnp.int32)[:, None]
    fraction = depth_frac[None, :]
    hat_basis = jnp.where(levels == knot_bin[None, :], 1.0 - fraction, 0.0)
    hat_basis = hat_basis + jnp.where(levels == knot_bin[None, :] + 1, fraction, 0.0)
    return jnp.concatenate([hat_basis, cell_covariates], axis=0)


def newton_solve(gram_flat, score):
    columns = score.shape[-1]
    identity = jnp.eye(columns, dtype=gram_flat.dtype)
    system = gram_flat.reshape(-1, columns, columns) + ridge_weight * identity
    factor_lower = jnp.linalg.cholesky(system)
    middle = jax.scipy.linalg.solve_triangular(factor_lower, score[..., None], lower=True)
    return jax.scipy.linalg.solve_triangular(factor_lower, middle, lower=True, trans=1)[..., 0]


def local_plain(
    counts,
    batch_id,
    live_cells,
    knot_bin,
    depth_frac,
    cell_covariates,
    coefficients,
    batch_effect,
    factors,
    loadings,
):
    highest = lax.Precision.HIGHEST
    contract = (((1,), (1,)), ((), ()))
    observed = counts.astype(jnp.float32)
    totals = lax.psum(jnp.sum(observed, axis=0), "gene")
    offset = jnp.log((1.0 + totals) / GENES)
    slot_count = observed.shape[1]
    live_mask = (jnp.arange(slot_count, dtype=jnp.int32) < live_cells[0]).astype(jnp.float32)
    design = design_rows(knot_bin, depth_frac, cell_covariates)
    columns = design.shape[0]
    onehot = (jnp.arange(BATCHES, dtype=jnp.int32)[:, None] == batch_id[None, :]).astype(
        jnp.float32
    )
    stacked = jnp.concatenate([design, onehot], axis=0)
    linear = jnp.dot(
        jnp.concatenate([coefficients, batch_effect], axis=1), stacked, precision=highest
    )
    latent = lax.dot_general(loadings, factors, contract, preferred_element_type=jnp.float32)
    linear_pred = offset[None, :] + linear + latent
    expected = jnp.exp(linear_pred)
    weight = expected * live_mask
    residual = (observed - expected) * live_mask
    pairs = (design[:, None, :] * design[None, :, :]).reshape(columns * columns, slot_count)
    gram_part = lax.dot_general(weight, pairs, contract, precision=highest)
    score_part = lax.dot_general(residual, design, contract, precision=highest)
    gram_share, score_share = (
        lax.psum_scatter(gram_part, "cell", scatter_dimension=0, tiled=True),
        lax.psum_scatter(score_part, "cell", scatter_dimension=0, tiled=True),
    )
    step_share = newton_solve(gram_share, score_share)
    beta_step = lax.all_gather(step_share, "cell", axis=0, tiled=True)
    expected_next = jnp.exp(linear_pred + jnp.dot(beta_step, design, precision=highest))
    weight_next = expected_next * live_mask
    residual_next = (observed - expected_next) * live_mask
    factors_wide = factors.astype(jnp.float32)
    loads_wide = loadings.astype(jnp.float32)
    grad_load = jnp.dot(residual_next, factors_wide, precision=highest)
    curv_load = jnp.dot(weight_next, factors_wide * factors_wide, precision=highest)
    back = (((0,), (0,)), ((), ()))
    grad_fact = lax.dot_general(residual_next, loads_wide, back, precision=highest)
    curv_fact = lax.dot_general(weight_next, loads_wide * loads_wide, back, precision=highest)
    grad_load, curv_load = lax.psum((grad_load, curv_load), "cell")
    grad_fact, curv_fact = lax.psum((grad_fact, curv_fact), "gene")
    factor_step = grad_fact / (curv_fact + 1.0)
    loading_score = grad_load / jnp.sqrt(curv_load + 1.0)
    return (beta_step, factor_step, loading_score)


MESH = pl.DeviceIdType.MESH
F32, BF16 = jnp.float32, jnp.bfloat16
VM = pl.BlockSpec(memory_space=pltpu.VMEM)
ROWS_BY_ROWS = (((1,), (1,)), ((), ()))
ACROSS = (((1,), (0,)), ((), ()))
DOWN = (((0,), (0,)), ((), ()))
LIMIT = 60 * 1024 * 1024


def split(x):
    high = x.astype(BF16)
    return high, (x - high.astype(F32)).astype(BF16)


def mul(a, b, dims):
    return lax.dot_general(a, b, dims, preferred_element_type=F32)


def remote(src, dst, send, recv, where):
    return pltpu.make_async_remote_copy(
        src_ref=src, dst_ref=dst, send_sem=send, recv_sem=recv, device_id=where, device_id_type=MESH
    )


def meet(groups):
    barrier = pltpu.get_barrier_semaphore()
    count = 0
    for axis, n in groups:
        me = lax.axis_index(axis)
        for d in range(1, n):
            pl.semaphore_signal(
                barrier, inc=1, device_id={axis: lax.rem(me + d, n)}, device_id_type=MESH
            )
        count += n - 1
    pl.semaphore_wait(barrier, count)


def totals_kernel(n, x_ref, o_ref, recv, send_sem, recv_sem):
    me = lax.axis_index("gene")
    meet((("gene", n),))
    copies = []
    for d in range(1, n):
        copies.append(
            remote(
                x_ref, recv.at[d - 1], send_sem.at[d - 1], recv_sem.at[d - 1],
                {"gene": lax.rem(me + d, n)},
            )
        )
        copies[-1].start()
    total = x_ref[...]
    for d in range(1, n):
        copies[d - 1].wait()
        total = total + recv[d - 1]
    o_ref[...] = total


def design_of(knot_ref, frac_ref, cov_ref):
    slots = knot_ref.shape[1]
    levels = lax.broadcasted_iota(jnp.int32, (SPL, slots), 0)
    knot, frac = knot_ref[...], frac_ref[...]
    hats = jnp.where(levels == knot, 1.0 - frac, 0.0)
    hats = hats + jnp.where(levels == knot + 1, frac, 0.0)
    return hats, cov_ref[...]


def first_kernel(
    counts_ref, totals_ref, batch_ref, live_ref, knot_ref, frac_ref, cov_ref, coef_ref, shift_ref,
    factors_ref, loads_ref, g_ref, lin_ref, rhs, pair_hi, pair_lo, des_hi, des_lo, extra,
):
    slots = counts_ref.shape[1]

    @pl.when(pl.program_id(0) == 0)
    def _():
        hats, cov = design_of(knot_ref, frac_ref, cov_ref)
        ncov = cov.shape[0]
        half = ncov // 2
        design_hi, design_lo = split(jnp.concatenate([hats, cov], axis=0))
        hot = lax.broadcasted_iota(jnp.int32, (BATCHES, slots), 0) == batch_ref[...]
        hot = jnp.where(hot, 1.0, 0.0).astype(BF16)
        width = SPL + ncov
        rhs[0:width] = design_hi
        rhs[width : 2 * width] = design_hi
        rhs[2 * width : 3 * width] = design_lo
        rhs[3 * width : 3 * width + BATCHES] = hot
        rhs[3 * width + BATCHES : 3 * width + 2 * BATCHES] = hot
        rhs[3 * width + 2 * BATCHES :] = factors_ref[...]

        def put(at, block):
            high, low = split(block)
            pair_hi[at : at + block.shape[0]] = high
            pair_lo[at : at + block.shape[0]] = low

        at = 0
        for p in range(SPL):
            put(at, hats[p : p + 1] * cov)
            at += ncov
        for i in range(half):
            put(at, cov[i : i + 1] * cov)
            at += ncov
        for i in range(half, ncov, 2):
            put(
                at,
                jnp.concatenate(
                    [cov[i : i + 1] * cov[half:], cov[i + 1 : i + 2] * cov[half:]], axis=0
                ),
            )
            at += ncov
        put(at, hats * hats)
        at += SPL
        later = jnp.concatenate([hats[1:], jnp.zeros((1, slots), F32)], axis=0)
        put(at, hats * later)
        at += SPL
        put(at, jnp.zeros((width, slots), F32))
        des_hi[...] = jnp.zeros(des_hi.shape, BF16)
        des_lo[...] = jnp.zeros(des_lo.shape, BF16)
        des_hi[128 - width : 128] = design_hi
        des_lo[128 - width : 128] = design_lo
        extra[0:1] = jnp.log((1.0 + totals_ref[...]) / GENES)
        places = lax.broadcasted_iota(jnp.int32, (1, slots), 1)
        extra[1:2] = jnp.where(places < live_ref[0], 1.0, 0.0)

    coef_hi, coef_lo = split(coef_ref[...])
    shift_hi, shift_lo = split(shift_ref[...])
    lhs = jnp.concatenate([coef_hi, coef_lo, coef_hi, shift_hi, shift_lo, loads_ref[...]], axis=0)
    linear = mul(lhs, rhs[...], DOWN) + extra[0:1]
    lin_ref[...] = linear
    mask = extra[1:2]
    expected = jnp.exp(linear)
    w_hi, w_lo = split(expected * mask)
    r_hi, r_lo = split((counts_ref[...].astype(F32) - expected) * mask)
    gram = mul(w_hi, pair_hi[...], ROWS_BY_ROWS)
    gram = gram + mul(w_hi, pair_lo[...], ROWS_BY_ROWS)
    gram = gram + mul(w_lo, pair_hi[...], ROWS_BY_ROWS)
    score = mul(r_hi, des_hi[...], ROWS_BY_ROWS)
    score = score + mul(r_hi, des_lo[...], ROWS_BY_ROWS)
    score = score + mul(r_lo, des_hi[...], ROWS_BY_ROWS)
    blocks, rows, wide = g_ref.shape
    g_ref[:, :, : wide - 128] = gram[:, : wide - 128].reshape(blocks, rows, wide - 128)
    g_ref[:, :, wide - 128 :] = (gram[:, wide - 128 :] + score).reshape(blocks, rows, 128)


def solve(g, x):
    half = SPL // 2
    cov_at, low_at, hat_at = SPL * SPL, SPL * SPL + half * SPL, SPL * SPL + half * SPL + half * half
    off_at, score_at = hat_at + SPL, hat_at + 2 * SPL
    spot = lax.broadcasted_iota(jnp.int32, (half, g.shape[1]), 0)

    def one(block, i):
        return block[i : i + 1]

    lo = {}
    hi = {}
    for i in range(SPL):
        unit = jnp.where(spot == i % half, ridge_weight, 0.0)
        if i < half:
            lo[i] = g[cov_at + i * SPL : cov_at + i * SPL + half] + unit
            hi[i] = g[cov_at + i * SPL + half : cov_at + (i + 1) * SPL]
        else:
            hi[i] = g[low_at + (i - half) * half : low_at + (i - half + 1) * half] + unit
    b_lo = g[score_at + SPL : score_at + SPL + half]
    b_hi = g[score_at + SPL + half : score_at + 2 * SPL]
    pivot_inv, edge, side_lo, side_hi, rest = [], [], [], [], []
    for p in range(SPL):
        d = g[hat_at + p : hat_at + p + 1] + ridge_weight
        u_lo = g[p * SPL : p * SPL + half]
        u_hi = g[p * SPL + half : (p + 1) * SPL]
        b = g[score_at + p : score_at + p + 1]
        if p > 0:
            ratio = edge[-1] * pivot_inv[-1]
            d = d - ratio * edge[-1]
            u_lo = u_lo - ratio * side_lo[-1]
            u_hi = u_hi - ratio * side_hi[-1]
            b = b - ratio * rest[-1]
        inv = 1.0 / d
        pivot_inv.append(inv)
        edge.append(g[off_at + p : off_at + p + 1])
        side_lo.append(u_lo)
        side_hi.append(u_hi)
        rest.append(b)
        scaled_lo, scaled_hi = u_lo * inv, u_hi * inv
        b_lo = b_lo - scaled_lo * b
        b_hi = b_hi - scaled_hi * b
        for i in range(SPL):
            if i < half:
                f = one(scaled_lo, i)
                lo[i] = lo[i] - f * u_lo
            else:
                f = one(scaled_hi, i - half)
            hi[i] = hi[i] - f * u_hi
    c_inv, c_rest = [], []
    for j in range(SPL):
        if j < half:
            inv = 1.0 / one(lo[j], j)
            b = one(b_lo, j)
            s_lo = lo[j] * inv
            b_lo = b_lo - s_lo * b
        else:
            inv = 1.0 / one(hi[j], j - half)
            b = one(b_hi, j - half)
        s_hi = hi[j] * inv
        b_hi = b_hi - s_hi * b
        c_inv.append(inv)
        c_rest.append(b)
        for i in range(j + 1, SPL):
            if i < half:
                f = one(s_lo, i)
                lo[i] = lo[i] - f * lo[j]
            else:
                f = one(s_hi, i - half)
            hi[i] = hi[i] - f * hi[j]
    for j in reversed(range(SPL)):
        found = c_rest[j] * c_inv[j]
        x[SPL + j : SPL + j + 1] = found
        for i in range(j):
            c_rest[i] = c_rest[i] - (one(hi[i], j - half) if j >= half else one(lo[i], j)) * found
    x_lo, x_hi = x[SPL : SPL + half], x[SPL + half : 2 * SPL]
    after = None
    for p in reversed(range(SPL)):
        gone = jnp.sum(side_lo[p] * x_lo + side_hi[p] * x_hi, axis=0, keepdims=True)
        b = rest[p] - gone
        if after is not None:
            b = b - edge[p] * after
        after = b * pivot_inv[p]
        x[p : p + 1] = after


def newton_kernel(
    n, g_ref, o_ref, from_pair, to_far, from_far, tall, turned, mine, theirs,
    pair_send, pair_recv, far_send, far_recv, out_send, out_recv,
):
    me = lax.axis_index("cell")
    core, chip = lax.rem(me, 2), me // 2
    chips, rows, wide = n // 2, g_ref.shape[1], g_ref.shape[2]
    meet((("cell", n),))
    pair = []
    for d in list(range(1, chips)) + [0]:
        k = lax.rem(chip + d, chips)
        pair.append(
            remote(
                g_ref.at[2 * k + 1 - core], from_pair.at[d], pair_send.at[d], pair_recv.at[d],
                {"cell": me + 1 - 2 * core},
            )
        )
        pair[-1].start()
    far = []
    for d in range(1, chips):
        k = lax.rem(chip + d, chips)
        pair[d - 1].wait()
        to_far[d - 1] = g_ref[2 * k + core] + from_pair[d]
        far.append(
            remote(
                to_far.at[d - 1], from_far.at[d - 1], far_send.at[d - 1], far_recv.at[d - 1],
                {"cell": 2 * k + core},
            )
        )
        far[-1].start()
    pair[chips - 1].wait()
    total = g_ref[me] + from_pair[0]
    for d in range(1, chips):
        far[d - 1].wait()
        total = total + from_far[d - 1]
    tall[0:rows] = total
    if rows < 128:
        tall[rows:128] = jnp.zeros((128 - rows, wide), F32)
    turned[...] = tall[...].T
    solve(turned, mine)
    out = []
    for d in range(1, n):
        out.append(
            remote(
                mine, theirs.at[d - 1], out_send.at[d - 1], out_recv.at[d - 1],
                {"cell": lax.rem(me + d, n)},
            )
        )
        out[-1].start()
    width = mine.shape[0]
    fill = jnp.zeros((128 - width, 128), F32)

    def put(owner, block):
        o_ref[owner] = jnp.concatenate([block, fill], axis=0).T[:rows, :width]

    put(me, mine[...])
    for d in range(1, n):
        out[d - 1].wait()
        put(lax.rem(me + n - d, n), theirs[d - 1])


def spread(block):
    wide = block.astype(F32)
    zero = jnp.zeros(wide.shape, F32)
    square_hi, square_lo = split(jnp.concatenate([zero, wide * wide], axis=0))
    return jnp.concatenate([wide, zero], axis=0).astype(BF16), square_hi, square_lo


def last_kernel(
    n, m, counts_ref, lin_ref, live_ref, knot_ref, frac_ref, cov_ref, beta_ref, factors_ref,
    loads_ref, ls_ref, fs_ref, rhs, mask_ref, f_one, f_hi, f_lo, gl_ref, gf_ref,
    from_c, my_l, their_l, from_g, my_f, their_f,
    c_send, c_recv, g_send, g_recv, l_send, l_recv, f_send, f_recv,
):
    cell, gene = lax.axis_index("cell"), lax.axis_index("gene")
    half = gl_ref.shape[2] // 2
    span = gf_ref.shape[2]
    slots = counts_ref.shape[1]
    hats, cov = design_of(knot_ref, frac_ref, cov_ref)
    design_hi, design_lo = split(jnp.concatenate([hats, cov], axis=0))
    width = design_hi.shape[0]
    rhs[0:width] = design_hi
    rhs[width : 2 * width] = design_hi
    rhs[2 * width : 3 * width] = design_lo
    places = lax.broadcasted_iota(jnp.int32, (1, slots), 1)
    mask_ref[0:1] = jnp.where(places < live_ref[...], 1.0, 0.0)
    f_one[...], f_hi[...], f_lo[...] = spread(factors_ref[...])
    blocks, rows, _ = beta_ref.shape
    beta_hi, beta_lo = split(beta_ref[...].reshape(blocks * rows, width))
    lhs = jnp.concatenate([beta_hi, beta_lo, beta_hi], axis=1)
    l_one, l_hi, l_lo = spread(loads_ref[...])
    meet((("cell", n), ("gene", m)))
    across, along = [], []
    for d in list(range(1, m)) + [0]:
        to = lax.rem(gene + d, m)
        cols = pl.ds(pl.multiple_of(to * span, span), span)
        delta = mul(lhs, rhs[:, cols], ACROSS)
        mask = mask_ref[0:1, cols]
        expected = jnp.exp(lin_ref[:, cols] + delta)
        w_hi, w_lo = split(expected * mask)
        r_hi, r_lo = split((counts_ref[:, cols].astype(F32) - expected) * mask)
        gf = mul(l_one, r_hi, ACROSS) + mul(l_one, r_lo, ACROSS)
        gf = gf + mul(l_hi, w_hi, ACROSS) + mul(l_lo, w_hi, ACROSS) + mul(l_hi, w_lo, ACROSS)
        gf_ref[d] = gf
        if d > 0:
            along.append(
                remote(
                    gf_ref.at[d], from_g.at[d - 1], g_send.at[d - 1], g_recv.at[d - 1],
                    {"gene": to},
                )
            )
            along[-1].start()
        one, high, low = f_one[:, cols], f_hi[:, cols], f_lo[:, cols]
        gl = mul(r_hi, one, ROWS_BY_ROWS) + mul(r_lo, one, ROWS_BY_ROWS)
        gl = gl + mul(w_hi, high, ROWS_BY_ROWS)
        gl = gl + mul(w_hi, low, ROWS_BY_ROWS) + mul(w_lo, high, ROWS_BY_ROWS)
        gl = gl.reshape(gl_ref.shape)
        if d == 1:
            gl_ref[...] = gl
        else:
            gl_ref[...] += gl
    for d in range(1, n):
        to = lax.rem(cell + d, n)
        across.append(
            remote(gl_ref.at[to], from_c.at[d - 1], c_send.at[d - 1], c_recv.at[d - 1], {"cell": to})
        )
        across[-1].start()
    total = gl_ref[cell]
    for d in range(1, n):
        across[d - 1].wait()
        total = total + from_c[d - 1]
    my_l[...] = total[:, :half] / jnp.sqrt(total[:, half:] + 1.0)
    their_l[cell] = my_l[...]
    out_l, out_f = [], []
    for d in range(1, n):
        out_l.append(
            remote(
                my_l, their_l.at[cell], l_send.at[d - 1], l_recv.at[d - 1],
                {"cell": lax.rem(cell + d, n)},
            )
        )
        out_l[-1].start()
    total = gf_ref[0]
    for d in range(1, m):
        along[d - 1].wait()
        total = total + from_g[d - 1]
    my_f[...] = total[:half] / (total[half:] + 1.0)
    for d in range(1, m):
        out_f.append(
            remote(
                my_f, their_f.at[d - 1], f_send.at[d - 1], f_recv.at[d - 1],
                {"gene": lax.rem(gene + d, m)},
            )
        )
        out_f[-1].start()
    def put(owner, block):
        fs_ref[:, pl.ds(pl.multiple_of(owner * span, span), span)] = block

    put(gene, my_f[...])
    for d in range(1, n):
        out_l[d - 1].wait()
    found = their_l[...].reshape(ls_ref.shape[1], half)
    ls_ref[...] = jnp.concatenate([found, jnp.zeros(found.shape, F32)], axis=1).T[:half]
    for d in range(1, m):
        out_f[d - 1].wait()
        put(lax.rem(gene + m - d, m), their_f[d - 1])


def local_fused(
    n, m, counts, batch_id, live_cells, knot_bin, depth_frac, cell_covariates, coefficients,
    batch_effect, factors, loadings,
):
    genes, slots = counts.shape
    rows, span, latent = genes // n, slots // m, factors.shape[1]
    ncov = cell_covariates.shape[0]
    width = SPL + ncov
    wide = SPL * ncov + ncov * ncov * 3 // 4 + 2 * SPL + width
    steps = 2
    tile, blocks = genes // steps, n // steps
    dma = pltpu.SemaphoreType.DMA
    shape = jax.ShapeDtypeStruct

    def params(**kw):
        return pltpu.CompilerParams(vmem_limit_bytes=LIMIT, **kw)

    part = jnp.sum(counts, axis=0, keepdims=True).astype(F32)
    totals = pl.pallas_call(
        functools.partial(totals_kernel, m),
        out_shape=shape((1, slots), F32),
        in_specs=[VM],
        out_specs=VM,
        scratch_shapes=[pltpu.VMEM((m - 1, 1, slots), F32), dma((m - 1,)), dma((m - 1,))],
        compiler_params=params(collective_id=0, has_side_effects=True),
        name="totals",
    )(part)

    def by_rows(*tail):
        return pl.BlockSpec((tile,) + tail, lambda i: (i,) + (0,) * len(tail))

    def by_lanes(count):
        return pl.BlockSpec((count, tile), lambda i: (0, i))

    def by_blocks(*tail):
        return pl.BlockSpec((blocks,) + tail, lambda i: (i,) + (0,) * len(tail))

    def whole(*dims):
        return pl.BlockSpec(dims, lambda i: (0,) * len(dims))

    smem = pl.BlockSpec(memory_space=pltpu.SMEM)
    knot, frac, batch = (v.reshape(1, slots) for v in (knot_bin, depth_frac, batch_id))
    line = whole(1, slots)
    gram, lin = pl.pallas_call(
        first_kernel,
        grid=(steps,),
        out_shape=(shape((n, rows, wide), F32), shape((genes, slots), F32)),
        in_specs=[
            by_rows(slots), line, line, smem, line, line, whole(ncov, slots),
            by_lanes(width), by_lanes(BATCHES), whole(latent, slots), by_lanes(latent),
        ],
        out_specs=(by_blocks(rows, wide), by_rows(slots)),
        scratch_shapes=[
            pltpu.VMEM((3 * width + 2 * BATCHES + latent, slots), BF16),
            pltpu.VMEM((wide, slots), BF16),
            pltpu.VMEM((wide, slots), BF16),
            pltpu.VMEM((128, slots), BF16),
            pltpu.VMEM((128, slots), BF16),
            pltpu.VMEM((8, slots), F32),
        ],
        compiler_params=params(),
        name="first",
    )(
        counts, totals, batch, live_cells, knot, frac, cell_covariates, coefficients.T,
        batch_effect.T, factors.T, loadings.T,
    )
    chips = n // 2
    beta = pl.pallas_call(
        functools.partial(newton_kernel, n),
        out_shape=shape((n, rows, width), F32),
        in_specs=[VM],
        out_specs=VM,
        scratch_shapes=[
            pltpu.VMEM((chips, rows, wide), F32),
            pltpu.VMEM((chips - 1, rows, wide), F32),
            pltpu.VMEM((chips - 1, rows, wide), F32),
            pltpu.VMEM((128, wide), F32),
            pltpu.VMEM((wide, 128), F32),
            pltpu.VMEM((width, 128), F32),
            pltpu.VMEM((n - 1, width, 128), F32),
            dma((chips,)), dma((chips,)), dma((chips - 1,)), dma((chips - 1,)),
            dma((n - 1,)), dma((n - 1,)),
        ],
        compiler_params=params(collective_id=1, has_side_effects=True),
        name="newton",
    )(gram)
    ls, fs = pl.pallas_call(
        functools.partial(last_kernel, n, m),
        out_shape=(shape((latent, genes), F32), shape((latent, slots), F32)),
        in_specs=[VM] * 9,
        out_specs=(VM, VM),
        scratch_shapes=[
            pltpu.VMEM((3 * width, slots), BF16),
            pltpu.VMEM((8, slots), F32),
            pltpu.VMEM((2 * latent, slots), BF16),
            pltpu.VMEM((2 * latent, slots), BF16),
            pltpu.VMEM((2 * latent, slots), BF16),
            pltpu.VMEM((n, rows, 2 * latent), F32),
            pltpu.VMEM((m, 2 * latent, span), F32),
            pltpu.VMEM((n - 1, rows, 2 * latent), F32),
            pltpu.VMEM((rows, latent), F32),
            pltpu.VMEM((n, rows, latent), F32),
            pltpu.VMEM((m - 1, 2 * latent, span), F32),
            pltpu.VMEM((latent, span), F32),
            pltpu.VMEM((m - 1, latent, span), F32),
            dma((n - 1,)), dma((n - 1,)), dma((m - 1,)), dma((m - 1,)),
            dma((n - 1,)), dma((n - 1,)), dma((m - 1,)), dma((m - 1,)),
        ],
        compiler_params=params(collective_id=2, has_side_effects=True),
        name="last",
    )(
        counts, lin, live_cells.reshape(1, 1), knot, frac, cell_covariates, beta,
        factors.T, loadings.T,
    )
    return beta.reshape(genes, width), fs.T, ls.T


def local(n, m, *args):
    counts, cov, factors = args[0], args[5], args[8]
    genes, slots = counts.shape
    fits = (
        n % 2 == 0
        and n > 2
        and m > 1
        and genes % (16 * n) == 0
        and genes // n <= 128
        and slots % (128 * m) == 0
        and cov.shape[0] == SPL
        and factors.shape[1] == 64
    )
    if fits:
        return local_fused(n, m, *args)
    return local_plain(*args)


def solution(mesh):
    placed = (
        P("gene", "cell"),
        P("cell"),
        P("cell"),
        P("cell"),
        P("cell"),
        P(None, "cell"),
        P("gene", None),
        P("gene", None),
        P("cell", None),
        P("gene", None),
    )
    return jax.shard_map(
        functools.partial(local, mesh.shape["cell"], mesh.shape["gene"]),
        mesh=mesh,
        in_specs=placed,
        out_specs=(P("gene", None), P("cell", None), P("gene", None)),
        check_vma=False,
    )
```
